1024 devices in a mesh: section: 32 (over z_lo, x), dp: 32 (over y, z_hi, core).
Axes of the slice: x: 4, y: 4, z: 32 (z_hi: 4, z_lo: 8; z = z_hi * 8 + z_lo), core: 2. Of those that a mesh axis runs over, the one named last changes fastest.
Arguments:
- states: bfloat16 [32, 32, 32, 4096], P('dp', 'section'), may hold values from -8 to 8
- memory: bfloat16 [32, 32, 2, 128, 4096], P('dp', 'section'), may hold values from -12 to 12
- memory_len: int32 [32, 32], P('dp', 'section'), may hold values from 2 to 128
- decode_len: int32 [32, 32], P('dp', 'section'), may hold values from 1 to 32
- owner_map: int32 [32], replicated, may hold values from 0 to 31, as said below
- section_gain: bfloat16 [32, 4096], P('section'), may hold values from 0.5 to 2
- cotangent: bfloat16 [32, 3, 32, 32, 4096], P('dp', None, 'section'), may hold values from -18 to 18
Outputs:
- final_states: bfloat16 [32, 32, 32, 4096], P('dp', 'section')
- gain_grad: float32 [32, 4096], P('section')
The draws below stay inside these ranges and needn't reach their ends.
Inputs may be any that keep to these rules, and one draw needn't show every extreme that they name: owner_map[m] = (m + c) mod 32 for one offset c from 3 to 31, the same for all m.
All inputs are finite; a program needn't handle non-finite values.
Results may differ from the reference program's by a relative error of at most 0.0085.
Values may be sent and summed in bfloat16 or wider, within the bound.
No kernel may reach another device: no remote copies, remote signals or barrier semaphores. Data moves between devices by JAX's collectives and lax.ppermute only.
A program may use at most 32 MiB of HBM per device.

```python
import jax
import jax.numpy as jnp
from jax import lax

HEADS = 16
HD = 256
D = 4096
DEC = 32
ENC = 128
STEPS = 3
REPLICAS = 32
SECTIONS = 32


def draw_owner_map(key, part):
    offset = jax.random.randint(jax.random.fold_in(key, 51), (), STEPS, SECTIONS)
    return ((jnp.arange(SECTIONS) + offset) % SECTIONS).astype(jnp.int32)


def draw_states(key, part):
    shape_all = (REPLICAS, SECTIONS, DEC, HEADS * HD)
    own = jax.random.fold_in(key, 21)
    values = jnp.clip(jax.random.normal(own, shape_all, jnp.float32), -6.0, 6.0)
    return values.astype(jnp.bfloat16)


def draw_memory(key, part):
    shape_half = (REPLICAS, SECTIONS, ENC, HEADS * HD)
    key_seed = jax.random.fold_in(key, 31)
    value_seed = jax.random.fold_in(key, 32)
    keys = jnp.clip(2.0 * jax.random.normal(key_seed, shape_half, jnp.float32), -12.0, 12.0).astype(jnp.bfloat16)
    values = jnp.clip(2.0 * jax.random.normal(value_seed, shape_half, jnp.float32), -12.0, 12.0).astype(jnp.bfloat16)
    return jnp.stack([keys, values], axis=2)


def draw_cotangent(key, part):
    shape_all = (REPLICAS, STEPS, SECTIONS, DEC, HEADS * HD)
    own = jax.random.fold_in(key, 41)
    rising = 3.0 ** (jnp.arange(REPLICAS, dtype=jnp.float32) / max(REPLICAS - 1, 1))
    rising = rising.reshape(REPLICAS, 1, 1, 1, 1)
    values = jnp.clip(jax.random.normal(own, shape_all, jnp.float32), -6.0, 6.0)
    return (values * rising).astype(jnp.bfloat16)


def touch_ends(array, stream_key, low, high):
    index_at = [jax.random.randint(jax.random.fold_in(stream_key, axis), (), 0, length) for axis, length in enumerate(array.shape)]
    longest = array.shape.index(max(array.shape))
    next_to = index_at[:longest] + [(index_at[longest] + 1) % array.shape[longest]] + index_at[longest + 1:]
    return array.at[tuple(index_at)].set(low).at[tuple(next_to)].set(high)


def level_of(rng, extent, shards, least, largest):
    loudness, own = 1.0, jax.random.fold_in(rng, 6)
    for axis_at, parts in shards:
        steps = jnp.exp(jax.random.uniform(jax.random.fold_in(own, axis_at), (parts,), jnp.float32, least / len(shards), largest / len(shards)))
        loudness = loudness * jnp.repeat(steps, extent[axis_at] // parts).reshape([-1 if axis == axis_at else 1 for axis in range(len(extent))])
    return loudness


def setup_inputs(seed: int = 0) -> dict:
    key_of = jax.random.split(jax.random.key(seed), 8)
    states = draw_states(jax.random.fold_in(key_of[7], 71), 0)
    memory = draw_memory(jax.random.fold_in(key_of[7], 71), 0)
    memory_len = touch_ends(jax.random.randint(key_of[2], (REPLICAS, SECTIONS), 2, ENC + 1), jax.random.fold_in(key_of[2], 1), 2, ENC).astype(jnp.int32)
    decode_len = touch_ends(jax.random.randint(key_of[3], (REPLICAS, SECTIONS), 1, DEC + 1), jax.random.fold_in(key_of[3], 1), 1, DEC).astype(jnp.int32)
    owner_map = draw_owner_map(jax.random.fold_in(key_of[7], 71), 0)
    section_gain = jnp.clip(0.5 + 1.5 * jax.random.uniform(key_of[5], (SECTIONS, D), jnp.float32) ** level_of(key_of[5], (SECTIONS, D), ((0, 32),), -0.2, 0.2), 0.5, 2.0).astype(jnp.bfloat16)
    cotangent = draw_cotangent(jax.random.fold_in(key_of[7], 71), 0)
    return dict(states=states, memory=memory, memory_len=memory_len, decode_len=decode_len, owner_map=owner_map, section_gain=section_gain, cotangent=cotangent)


def attend(queries, key_rows, value_rows, memory_length):
    sections_here = queries.shape[0]
    query_heads = queries.astype(jnp.float32).reshape(sections_here, DEC, HEADS, HD)
    key_heads = key_rows.astype(jnp.float32).reshape(sections_here, ENC, HEADS, HD)
    value_heads = value_rows.astype(jnp.float32).reshape(sections_here, ENC, HEADS, HD)
    scores = jnp.einsum('sqhd,skhd->shqk', query_heads, key_heads) * HD ** (-0.5)
    key_live = jnp.arange(ENC)[None, :] < memory_length[:, None]
    scores = jnp.where(key_live[:, None, None, :], scores, jnp.float32(-1e+30))
    top = lax.optimization_barrier(jnp.max(scores, axis=-1, keepdims=True))
    expo = jnp.exp(scores - top)
    probs = (expo / lax.optimization_barrier(jnp.sum(expo, axis=-1, keepdims=True))).astype(jnp.bfloat16)
    mixed = jnp.einsum('shqk,skhd->sqhd', probs.astype(jnp.float32), value_heads)
    return mixed.reshape(sections_here, DEC, HEADS * HD).astype(jnp.bfloat16)

def reference(states, memory, memory_len, decode_len, owner_map, section_gain, cotangent):

    def one_replica(pieces):
        current, memory_rep, memory_rep_len, decode_rep_len, cotangent_rep = pieces
        held = memory_rep[owner_map]
        held_len = memory_rep_len[owner_map]
        gain_total = jnp.zeros((SECTIONS, HEADS * HD), jnp.float32)
        live_rows = jnp.arange(DEC)[None, :, None] < decode_rep_len[:, None, None]
        for window_step in range(STEPS):
            state_wide = current.astype(jnp.float32)
            queries = (state_wide * lax.rsqrt(lax.optimization_barrier(jnp.mean(state_wide * state_wide, axis=-1, keepdims=True)) + 1e-06)).astype(jnp.bfloat16)
            attended = attend(queries, held[:, 0], held[:, 1], held_len).astype(jnp.float32)
            gains_now = jnp.roll(section_gain, -window_step, 0).astype(jnp.float32)[:, None, :]
            cot_now = jnp.roll(cotangent_rep[window_step], -window_step, 0).astype(jnp.float32)
            by_batch = lax.optimization_barrier(jnp.sum(jnp.where(live_rows, cot_now * attended, jnp.float32(0.0)), axis=1))
            gain_total = gain_total + jnp.roll(by_batch, window_step, 0)
            current = jnp.where(live_rows, state_wide + gains_now * attended, state_wide).astype(jnp.bfloat16)
        return (jnp.roll(current, STEPS - 1, 0), gain_total)
    finals, totals = lax.map(one_replica, (states, memory, memory_len, decode_len, cotangent))
    return (finals, lax.optimization_barrier(jnp.sum(totals, axis=0)))
```

```python
import jax
import jax.numpy as jnp
from jax import lax
from jax.sharding import PartitionSpec as P

HD = 256
STEPS = 3
LEAST_OFFSET = 3
CORES = 2
ROWS_Y = 4


def shifted(value, axis, steps):
    count = lax.axis_size(axis)
    pairs = [(source, (source + steps) % count) for source in range(count)]
    return lax.ppermute(value, axis, pairs)


def attend(queries, key_rows, value_rows, key_live):
    rows_here = queries.shape[0]
    width = queries.shape[1]
    heads_here = width // HD
    query_heads = queries.reshape(rows_here, heads_here, HD)
    key_heads = key_rows.reshape(key_rows.shape[0], heads_here, HD)
    value_heads = value_rows.reshape(value_rows.shape[0], heads_here, HD)
    scores = jnp.einsum(
        "qhd,khd->hqk", query_heads, key_heads, preferred_element_type=jnp.float32
    ) * HD ** (-0.5)
    scores = jnp.where(key_live[None, None, :], scores, jnp.float32(-1e30))
    top = jnp.max(scores, axis=-1, keepdims=True)
    expo = jnp.exp(scores - top)
    probs = (expo / jnp.sum(expo, axis=-1, keepdims=True)).astype(jnp.bfloat16)
    mixed = jnp.einsum("hqk,khd->qhd", probs, value_heads, preferred_element_type=jnp.float32)
    return mixed.reshape(rows_here, width).astype(jnp.bfloat16)


def normalized(state_wide):
    return (
        state_wide * lax.rsqrt(jnp.mean(state_wide * state_wide, axis=-1, keepdims=True) + 1e-06)
    ).astype(jnp.bfloat16)


def updated(state, gain, attended):
    return (
        state.astype(jnp.float32) + gain.astype(jnp.float32)[None, :] * attended.astype(jnp.float32)
    ).astype(jnp.bfloat16)


def dp_sum(row):
    count = lax.axis_size("dp")
    runs = count // ROWS_Y

    def partner(source, stage, j):
        y, rest = divmod(source, runs)
        run, core = divmod(rest, CORES)
        if stage == 0:
            core = (core + j) % CORES
        elif stage == 1:
            y = (y + j) % ROWS_Y
        else:
            run = (run + j) % (runs // CORES)
        return y * runs + run * CORES + core

    for stage, size in enumerate((CORES, ROWS_Y, runs // CORES)):
        arrived = [
            lax.ppermute(row, "dp", [(s, partner(s, stage, j)) for s in range(count)])
            for j in range(1, size)
        ]
        for piece in arrived:
            row = row + piece
    return row


def by_offset(offset_index, sections, send, *operands):
    def branch(offset):
        return lambda *values: send(offset, *values)

    return lax.switch(
        offset_index, [branch(c) for c in range(LEAST_OFFSET, sections)], *operands
    )


def to_owner(offset, states, gain, length):
    length_row = jnp.full((128,), length, jnp.int32).astype(jnp.bfloat16)
    return (
        shifted(states, "section", offset),
        shifted(jnp.concatenate([gain, length_row]), "section", offset),
        shifted(gain, "section", offset - 1),
    )


def from_owner(offset, *attended):
    return tuple(shifted(a, "section", t - offset) for t, a in enumerate(attended))


def per_device(states, memory, memory_len, decode_len, owner_map, section_gain, cotangent):
    sections = lax.axis_size("section")
    state, gain = states[0, 0], section_gain[0]
    keys, values = memory[0, 0, 0], memory[0, 0, 1]
    width = state.shape[1]
    key_live = jnp.arange(keys.shape[0]) < memory_len[0, 0]
    row_index = jnp.arange(state.shape[0])[:, None]
    offset_index = owner_map[0] - LEAST_OFFSET

    current, aux, gain_next = by_offset(
        offset_index, sections, to_owner, state, gain, decode_len[0, 0]
    )
    gains = [aux[:width], gain_next]
    live = row_index < aux[width].astype(jnp.int32)
    sent = []
    for t in range(STEPS):
        attended = attend(normalized(current.astype(jnp.float32)), keys, values, key_live)
        attended = jnp.where(live, attended, jnp.bfloat16(0))
        sent.append(attended)
        if t + 1 < STEPS:
            current = updated(current, gains[t], attended)
    sent = by_offset(offset_index, sections, from_owner, *sent)
    total = jnp.zeros((width,), jnp.float32)
    for t in range(STEPS):
        total = total + jnp.sum(
            cotangent[0, t, 0].astype(jnp.float32) * sent[t].astype(jnp.float32), axis=0
        )
    summed = dp_sum(total[None])
    for t in range(STEPS):
        state = updated(state, gain, sent[t])
        if t + 1 < STEPS:
            state = shifted(state, "section", 1)
    return (state[None, None], summed)


def solution(mesh):
    in_specs = (
        P("dp", "section", None, None),
        P("dp", "section", None, None, None),
        P("dp", "section"),
        P("dp", "section"),
        P(),
        P("section", None),
        P("dp", None, "section", None, None),
    )
    out_specs = (P("dp", "section", None, None), P("section", None))
    return jax.shard_map(
        per_device, mesh=mesh, in_specs=in_specs, out_specs=out_specs, check_vma=False
    )
```

```python
import functools

import jax
import jax.numpy as jnp
from jax import lax
from jax.experimental import pallas as pl
from jax.experimental.pallas import tpu as pltpu
from jax.sharding import PartitionSpec as P

HD = 256
STEPS = 3
LEAST_OFFSET = 3
LANES = 128
CORES = 2
ROWS_Y = 4
VMEM = pl.BlockSpec(memory_space=pltpu.VMEM)
SMEM = pl.BlockSpec(memory_space=pltpu.SMEM)


def shifted(value, axis, steps):
    count = lax.axis_size(axis)
    pairs = [(source, (source + steps) % count) for source in range(count)]
    return lax.ppermute(value, axis, pairs)


def pack_kernel(length_ref, state_ref, gain_ref, message_ref):
    blocks = state_ref.shape[1] // LANES
    for b in range(blocks):
        message_ref[b] = state_ref[:, b * LANES : (b + 1) * LANES]
    wide = gain_ref[...].astype(jnp.float32)
    rows = [wide[:, b * LANES : (b + 1) * LANES] for b in range(blocks)]
    message_ref[blocks] = jnp.concatenate(rows, axis=0).astype(jnp.bfloat16)
    length = jnp.full(message_ref.shape[1:], length_ref[0], jnp.int32)
    message_ref[blocks + 1] = length.astype(jnp.float32).astype(jnp.bfloat16)


def packed(states, gain, length):
    rows, width = states.shape
    blocks = width // LANES
    return pl.pallas_call(
        pack_kernel,
        out_shape=jax.ShapeDtypeStruct((blocks + 2, rows, LANES), states.dtype),
        in_specs=[SMEM, VMEM, VMEM],
        out_specs=VMEM,
        name="pack",
    )(length, states, gain)


def steps_kernel(key_len_ref, message_ref, gain_next_ref, memory_ref, *refs):
    out_refs, (score_ref, state_ref) = refs[:STEPS], refs[STEPS:]
    rows = message_ref.shape[1]
    width = memory_ref.shape[2]
    heads, keys = width // HD, memory_ref.shape[1]
    blocks = width // LANES
    per_head = HD // LANES
    key_live = lax.broadcasted_iota(jnp.int32, (rows, keys), 1) < key_len_ref[0]
    length = message_ref[blocks + 1][:, :1].astype(jnp.float32)
    row_live = lax.broadcasted_iota(jnp.int32, (rows, 1), 0).astype(jnp.float32) < length
    for t in range(STEPS):
        source = message_ref if t == 0 else state_ref
        squares = jnp.zeros((rows, LANES), jnp.float32)
        for b in range(blocks):
            wide = source[b].astype(jnp.float32)
            squares = squares + wide * wide
        mean = jnp.sum(squares, axis=1, keepdims=True) / width
        scale = lax.rsqrt(mean + 1e-06)
        for h in range(heads):
            query = jnp.concatenate(
                [
                    (source[h * per_head + j].astype(jnp.float32) * scale).astype(jnp.bfloat16)
                    for j in range(per_head)
                ],
                axis=1,
            )
            scores = lax.dot_general(
                query,
                memory_ref[0, :, h * HD : (h + 1) * HD],
                (((1,), (1,)), ((), ())),
                preferred_element_type=jnp.float32,
            )
            score_ref[h] = jnp.where(key_live, scores * HD ** (-0.5), jnp.float32(-1e30))
        for h in range(heads):
            scores = score_ref[h]
            expo = jnp.exp(scores - jnp.max(scores, axis=1, keepdims=True))
            probs = (expo / jnp.sum(expo, axis=1, keepdims=True)).astype(jnp.bfloat16)
            mixed = jnp.dot(
                probs,
                memory_ref[1, :, h * HD : (h + 1) * HD],
                preferred_element_type=jnp.float32,
            ).astype(jnp.bfloat16)
            mixed = jnp.where(row_live, mixed.astype(jnp.float32), 0.0)
            out_refs[t][:, h * HD : (h + 1) * HD] = mixed.astype(jnp.bfloat16)
            if t + 1 < STEPS:
                for j in range(per_head):
                    b = h * per_head + j
                    if t == 0:
                        gain = message_ref[blocks][b : b + 1, :]
                    else:
                        gain = gain_next_ref[:, b * LANES : (b + 1) * LANES]
                    state_ref[b] = (
                        source[b].astype(jnp.float32)
                        + gain.astype(jnp.float32) * mixed[:, j * LANES : (j + 1) * LANES]
                    ).astype(jnp.bfloat16)


def attended_steps(message, gain_next, memory, key_len):
    rows = message.shape[1]
    keys, width = memory.shape[1:]
    return pl.pallas_call(
        steps_kernel,
        out_shape=[jax.ShapeDtypeStruct((rows, width), jnp.bfloat16)] * STEPS,
        in_specs=[SMEM, VMEM, VMEM, VMEM],
        out_specs=[VMEM] * STEPS,
        scratch_shapes=[
            pltpu.VMEM((width // HD, rows, keys), jnp.float32),
            pltpu.VMEM((width // LANES, rows, LANES), jnp.bfloat16),
        ],
        compiler_params=pltpu.CompilerParams(vmem_limit_bytes=16 << 20),
        name="steps",
    )(key_len, message, gain_next, memory)


def updated(state, gain, attended):
    return (
        state.astype(jnp.float32) + gain.astype(jnp.float32) * attended.astype(jnp.float32)
    ).astype(jnp.bfloat16)


def by_offset(offset_index, sections, send, *operands):
    return lax.switch(
        offset_index,
        [functools.partial(send, c) for c in range(LEAST_OFFSET, sections)],
        *operands,
    )


def to_owner(offset, message, gain):
    return shifted(message, "section", offset), shifted(gain, "section", offset - 1)


def from_owner(offset, *attended):
    return tuple(shifted(a, "section", t - offset) for t, a in enumerate(attended))


def near_dp_sum(row):
    count = lax.axis_size("dp")
    runs = count // (ROWS_Y * CORES)
    groups = [
        [(y * runs + run) * CORES + core for y in range(ROWS_Y) for core in range(CORES)]
        for run in range(runs)
    ]
    copies = jnp.broadcast_to(row, (ROWS_Y * CORES, row.shape[1]))
    return jnp.sum(
        lax.all_to_all(copies, "dp", 0, 0, axis_index_groups=groups), axis=0, keepdims=True
    )


def from_run(row, step):
    count = lax.axis_size("dp")
    runs = count // (ROWS_Y * CORES)

    def target(source):
        y, rest = divmod(source, runs * CORES)
        run, core = divmod(rest, CORES)
        return (y * runs + (run + step) % runs) * CORES + core

    return lax.ppermute(row, "dp", [(s, target(s)) for s in range(count)])


def per_device(states, memory, memory_len, decode_len, owner_map, section_gain, cotangent):
    sections = lax.axis_size("section")
    runs = lax.axis_size("dp") // (ROWS_Y * CORES)
    state, gain = states[0, 0], section_gain
    offset_index = owner_map[0] - LEAST_OFFSET

    message = packed(state, gain, decode_len[0])
    message, gain_next = by_offset(offset_index, sections, to_owner, message, gain)
    sent = attended_steps(message, gain_next, memory[0, 0], memory_len[0])
    sent = by_offset(offset_index, sections, from_owner, *sent)

    total = jnp.zeros((1, state.shape[1]), jnp.float32)
    for t in range(STEPS):
        total = total + jnp.sum(
            cotangent[0, t, 0].astype(jnp.float32) * sent[t].astype(jnp.float32),
            axis=0,
            keepdims=True,
        )
    total, state = lax.optimization_barrier((total, updated(state, gain, sent[0])))
    state = shifted(state, "section", 1)
    total = near_dp_sum(total)
    arrived = [from_run(total, step) for step in range(1, runs)]
    state = shifted(updated(state, gain, sent[1]), "section", 1)
    state = updated(state, gain, sent[2])
    return (state[None, None], sum(arrived, total))


def solution(mesh):
    in_specs = (
        P("dp", "section", None, None),
        P("dp", "section", None, None, None),
        P("dp", "section"),
        P("dp", "section"),
        P(),
        P("section", None),
        P("dp", None, "section", None, None),
    )
    out_specs = (P("dp", "section", None, None), P("section", None))
    return jax.shard_map(
        per_device, mesh=mesh, in_specs=in_specs, out_specs=out_specs, check_vma=False
    )
```

```python
import functools

import jax
import jax.numpy as jnp
from jax import lax
from jax.experimental import pallas as pl
from jax.experimental.pallas import tpu as pltpu
from jax.sharding import PartitionSpec as P

HD = 256
STEPS = 3
LEAST_OFFSET = 3
LANES = 128
CORES = 2
ROWS_Y = 4
VMEM = pl.BlockSpec(memory_space=pltpu.VMEM)
SMEM = pl.BlockSpec(memory_space=pltpu.SMEM)


def shifted(value, axis, steps):
    count = lax.axis_size(axis)
    pairs = [(source, (source + steps) % count) for source in range(count)]
    return lax.ppermute(value, axis, pairs)


def pack_kernel(length_ref, state_ref, gain_ref, message_ref):
    blocks = state_ref.shape[1] // LANES
    for b in range(blocks):
        message_ref[b] = state_ref[:, b * LANES : (b + 1) * LANES]
    wide = gain_ref[...].astype(jnp.float32)
    rows = [wide[:, b * LANES : (b + 1) * LANES] for b in range(blocks)]
    message_ref[blocks] = jnp.concatenate(rows, axis=0).astype(jnp.bfloat16)
    length = jnp.full(message_ref.shape[1:], length_ref[0], jnp.int32)
    message_ref[blocks + 1] = length.astype(jnp.float32).astype(jnp.bfloat16)


def packed(states, gain, length):
    rows, width = states.shape
    blocks = width // LANES
    return pl.pallas_call(
        pack_kernel,
        out_shape=jax.ShapeDtypeStruct((blocks + 2, rows, LANES), states.dtype),
        in_specs=[SMEM, VMEM, VMEM],
        out_specs=VMEM,
        name="pack",
    )(length, states, gain)


def steps_kernel(key_len_ref, message_ref, gain_next_ref, memory_ref, *refs):
    out_refs, (score_ref, state_ref) = refs[:STEPS], refs[STEPS:]
    rows = message_ref.shape[1]
    width = memory_ref.shape[2]
    heads, keys = width // HD, memory_ref.shape[1]
    blocks = width // LANES
    per_head = HD // LANES
    key_live = lax.broadcasted_iota(jnp.int32, (rows, keys), 1) < key_len_ref[0]
    length = message_ref[blocks + 1][:, :1].astype(jnp.float32)
    row_live = lax.broadcasted_iota(jnp.int32, (rows, 1), 0).astype(jnp.float32) < length
    for t in range(STEPS):
        source = message_ref if t == 0 else state_ref
        squares = jnp.zeros((rows, LANES), jnp.float32)
        for b in range(blocks):
            wide = source[b].astype(jnp.float32)
            squares = squares + wide * wide
        mean = jnp.sum(squares, axis=1, keepdims=True) / width
        scale = lax.rsqrt(mean + 1e-06)
        for h in range(heads):
            query = jnp.concatenate(
                [
                    (source[h * per_head + j].astype(jnp.float32) * scale).astype(jnp.bfloat16)
                    for j in range(per_head)
                ],
                axis=1,
            )
            scores = lax.dot_general(
                query,
                memory_ref[0, :, h * HD : (h + 1) * HD],
                (((1,), (1,)), ((), ())),
                preferred_element_type=jnp.float32,
            )
            score_ref[h] = jnp.where(key_live, scores * HD ** (-0.5), jnp.float32(-1e30))
        for h in range(heads):
            scores = score_ref[h]
            expo = jnp.exp(scores - jnp.max(scores, axis=1, keepdims=True))
            probs = (expo / jnp.sum(expo, axis=1, keepdims=True)).astype(jnp.bfloat16)
            mixed = jnp.dot(
                probs,
                memory_ref[1, :, h * HD : (h + 1) * HD],
                preferred_element_type=jnp.float32,
            ).astype(jnp.bfloat16)
            mixed = jnp.where(row_live, mixed.astype(jnp.float32), 0.0)
            out_refs[t][:rows, h * HD : (h + 1) * HD] = mixed.astype(jnp.bfloat16)
            if t + 1 == STEPS:
                for j in range(per_head):
                    b = h * per_head + j
                    out_refs[t][rows:, b * LANES : (b + 1) * LANES] = source[b]
            else:
                for j in range(per_head):
                    b = h * per_head + j
                    if t == 0:
                        gain = message_ref[blocks][b : b + 1, :]
                    else:
                        gain = gain_next_ref[:, b * LANES : (b + 1) * LANES]
                    state_ref[b] = (
                        source[b].astype(jnp.float32)
                        + gain.astype(jnp.float32) * mixed[:, j * LANES : (j + 1) * LANES]
                    ).astype(jnp.bfloat16)


def attended_steps(message, gain_next, memory, key_len):
    rows = message.shape[1]
    keys, width = memory.shape[1:]
    return pl.pallas_call(
        steps_kernel,
        out_shape=[
            jax.ShapeDtypeStruct((rows * (1 + (t + 1 == STEPS)), width), jnp.bfloat16)
            for t in range(STEPS)
        ],
        in_specs=[SMEM, VMEM, VMEM, VMEM],
        out_specs=[VMEM] * STEPS,
        scratch_shapes=[
            pltpu.VMEM((width // HD, rows, keys), jnp.float32),
            pltpu.VMEM((width // LANES, rows, LANES), jnp.bfloat16),
        ],
        compiler_params=pltpu.CompilerParams(vmem_limit_bytes=16 << 20),
        name="steps",
    )(key_len, message, gain_next, memory)


def updated(state, gain, attended):
    return (
        state.astype(jnp.float32) + gain.astype(jnp.float32) * attended.astype(jnp.float32)
    ).astype(jnp.bfloat16)


def by_offset(offset_index, sections, send, *operands):
    return lax.switch(
        offset_index,
        [functools.partial(send, c) for c in range(LEAST_OFFSET, sections)],
        *operands,
    )


def to_owner(offset, message, gain):
    message = shifted(message, "section", offset)
    return message, shifted(gain, "section", offset - 1)


def from_owner(offset, *attended):
    return tuple(shifted(a, "section", t - offset) for t, a in enumerate(attended))


def near_dp_sum(row):
    count = lax.axis_size("dp")
    runs = count // (ROWS_Y * CORES)
    groups = [
        [(y * runs + run) * CORES + core for y in range(ROWS_Y) for core in range(CORES)]
        for run in range(runs)
    ]
    copies = jnp.broadcast_to(row, (ROWS_Y * CORES, row.shape[1]))
    return jnp.sum(
        lax.all_to_all(copies, "dp", 0, 0, axis_index_groups=groups), axis=0, keepdims=True
    )


def far_dp_sum(row):
    count = lax.axis_size("dp")
    runs = count // (ROWS_Y * CORES)
    groups = [
        [(y * runs + run) * CORES + core for run in range(runs)]
        for y in range(ROWS_Y)
        for core in range(CORES)
    ]
    return lax.psum(row, "dp", axis_index_groups=groups)


def per_device(states, memory, memory_len, decode_len, owner_map, section_gain, cotangent):
    sections = lax.axis_size("section")
    state, gain = states[0, 0], section_gain
    offset_index = owner_map[0] - LEAST_OFFSET

    message = packed(state, gain, decode_len[0])
    message, gain_next = by_offset(offset_index, sections, to_owner, message, gain)
    sent = attended_steps(message, gain_next, memory[0, 0], memory_len[0])
    sent = by_offset(offset_index, sections, from_owner, *sent)

    rows = state.shape[0]
    total = jnp.zeros((1, state.shape[1]), jnp.float32)
    for t in range(STEPS):
        total = total + jnp.sum(
            cotangent[0, t, 0].astype(jnp.float32) * sent[t][:rows].astype(jnp.float32),
            axis=0,
            keepdims=True,
        )
    state = updated(sent[-1][rows:], gain, sent[-1][:rows])
    return (state[None, None], far_dp_sum(near_dp_sum(total)))


def solution(mesh):
    in_specs = (
        P("dp", "section", None, None),
        P("dp", "section", None, None, None),
        P("dp", "section"),
        P("dp", "section"),
        P(),
        P("section", None),
        P("dp", None, "section", None, None),
    )
    out_specs = (P("dp", "section", None, None), P("section", None))
    return jax.shard_map(
        per_device, mesh=mesh, in_specs=in_specs, out_specs=out_specs, check_vma=False
    )
```

```python
import functools

import jax
import jax.numpy as jnp
from jax import lax
from jax.experimental import pallas as pl
from jax.experimental.pallas import tpu as pltpu
from jax.sharding import PartitionSpec as P

HD = 256
STEPS = 3
LEAST_OFFSET = 3
LANES = 128
CORES = 2
ROWS_Y = 4
VMEM = pl.BlockSpec(memory_space=pltpu.VMEM)
SMEM = pl.BlockSpec(memory_space=pltpu.SMEM)


def shifted(value, axis, steps):
    count = lax.axis_size(axis)
    pairs = [(source, (source + steps) % count) for source in range(count)]
    return lax.ppermute(value, axis, pairs)


def pack_kernel(length_ref, state_ref, gain_ref, message_ref):
    blocks = state_ref.shape[1] // LANES
    for b in range(blocks):
        message_ref[b] = state_ref[:, b * LANES : (b + 1) * LANES]
    wide = gain_ref[...].astype(jnp.float32)
    rows = [wide[:, b * LANES : (b + 1) * LANES] for b in range(blocks)]
    message_ref[blocks] = jnp.concatenate(rows, axis=0).astype(jnp.bfloat16)
    length = jnp.full(message_ref.shape[1:], length_ref[0], jnp.int32)
    message_ref[blocks + 1] = length.astype(jnp.float32).astype(jnp.bfloat16)


def packed(states, gain, length):
    rows, width = states.shape
    blocks = width // LANES
    return pl.pallas_call(
        pack_kernel,
        out_shape=jax.ShapeDtypeStruct((blocks + 2, rows, LANES), states.dtype),
        in_specs=[SMEM, VMEM, VMEM],
        out_specs=VMEM,
        name="pack",
    )(length, states, gain)


def steps_kernel(key_len_ref, message_ref, gain_next_ref, memory_ref, *refs):
    out_refs, (score_ref, state_ref) = refs[:STEPS], refs[STEPS:]
    rows = message_ref.shape[1]
    width = memory_ref.shape[2]
    heads, keys = width // HD, memory_ref.shape[1]
    blocks = width // LANES
    per_head = HD // LANES
    key_live = lax.broadcasted_iota(jnp.int32, (rows, keys), 1) < key_len_ref[0]
    length = message_ref[blocks + 1][:, :1].astype(jnp.float32)
    row_live = lax.broadcasted_iota(jnp.int32, (rows, 1), 0).astype(jnp.float32) < length
    for t in range(STEPS):
        source = message_ref if t == 0 else state_ref
        squares = jnp.zeros((rows, LANES), jnp.float32)
        for b in range(blocks):
            wide = source[b].astype(jnp.float32)
            squares = squares + wide * wide
        mean = jnp.sum(squares, axis=1, keepdims=True) / width
        scale = lax.rsqrt(mean + 1e-06)
        for h in range(heads):
            query = jnp.concatenate(
                [
                    (source[h * per_head + j].astype(jnp.float32) * scale).astype(jnp.bfloat16)
                    for j in range(per_head)
                ],
                axis=1,
            )
            scores = lax.dot_general(
                query,
                memory_ref[0, :, h * HD : (h + 1) * HD],
                (((1,), (1,)), ((), ())),
                preferred_element_type=jnp.float32,
            )
            score_ref[h] = jnp.where(key_live, scores * HD ** (-0.5), jnp.float32(-1e30))
        for h in range(heads):
            scores = score_ref[h]
            expo = jnp.exp(scores - jnp.max(scores, axis=1, keepdims=True))
            probs = (expo / jnp.sum(expo, axis=1, keepdims=True)).astype(jnp.bfloat16)
            mixed = jnp.dot(
                probs,
                memory_ref[1, :, h * HD : (h + 1) * HD],
                preferred_element_type=jnp.float32,
            ).astype(jnp.bfloat16)
            mixed = jnp.where(row_live, mixed.astype(jnp.float32), 0.0)
            out_refs[t][:, h * HD : (h + 1) * HD] = mixed.astype(jnp.bfloat16)
            if t + 1 < STEPS:
                for j in range(per_head):
                    b = h * per_head + j
                    if t == 0:
                        gain = message_ref[blocks][b : b + 1, :]
                    else:
                        gain = gain_next_ref[:, b * LANES : (b + 1) * LANES]
                    state_ref[b] = (
                        source[b].astype(jnp.float32)
                        + gain.astype(jnp.float32) * mixed[:, j * LANES : (j + 1) * LANES]
                    ).astype(jnp.bfloat16)


def attended_steps(message, gain_next, memory, key_len):
    rows = message.shape[1]
    keys, width = memory.shape[1:]
    return pl.pallas_call(
        steps_kernel,
        out_shape=[jax.ShapeDtypeStruct((rows, width), jnp.bfloat16)] * STEPS,
        in_specs=[SMEM, VMEM, VMEM, VMEM],
        out_specs=[VMEM] * STEPS,
        scratch_shapes=[
            pltpu.VMEM((width // HD, rows, keys), jnp.float32),
            pltpu.VMEM((width // LANES, rows, LANES), jnp.bfloat16),
        ],
        compiler_params=pltpu.CompilerParams(vmem_limit_bytes=16 << 20),
        name="steps",
    )(key_len, message, gain_next, memory)


def updated(state, gain, attended):
    return (
        state.astype(jnp.float32) + gain.astype(jnp.float32) * attended.astype(jnp.float32)
    ).astype(jnp.bfloat16)


def by_offset(offset_index, sections, send, *operands):
    return lax.switch(
        offset_index,
        [functools.partial(send, c) for c in range(LEAST_OFFSET, sections)],
        *operands,
    )


def to_owner(offset, message, gain):
    message = shifted(message, "section", offset)
    return message, shifted(gain, "section", offset - 1), shifted(gain, "section", 1)


def from_owner(offset, *attended):
    return tuple(shifted(a, "section", t - offset) for t, a in enumerate(attended))


def near_dp_sum(row):
    count = lax.axis_size("dp")
    runs = count // (ROWS_Y * CORES)
    groups = [
        [(y * runs + run) * CORES + core for y in range(ROWS_Y) for core in range(CORES)]
        for run in range(runs)
    ]
    copies = jnp.broadcast_to(row, (ROWS_Y * CORES, row.shape[1]))
    return jnp.sum(
        lax.all_to_all(copies, "dp", 0, 0, axis_index_groups=groups), axis=0, keepdims=True
    )


def far_dp_sum(row):
    count = lax.axis_size("dp")
    runs = count // (ROWS_Y * CORES)
    groups = [
        [(y * runs + run) * CORES + core for run in range(runs)]
        for y in range(ROWS_Y)
        for core in range(CORES)
    ]
    return lax.psum(row, "dp", axis_index_groups=groups)


def per_device(states, memory, memory_len, decode_len, owner_map, section_gain, cotangent):
    sections = lax.axis_size("section")
    state, gain = states[0, 0], section_gain
    offset_index = owner_map[0] - LEAST_OFFSET

    message = packed(state, gain, decode_len[0])
    message, gain_next, gain_before = by_offset(offset_index, sections, to_owner, message, gain)
    sent = attended_steps(message, gain_next, memory[0, 0], memory_len[0])
    sent = by_offset(offset_index, sections, from_owner, *sent)

    total = jnp.zeros((1, state.shape[1]), jnp.float32)
    for t in range(STEPS):
        total = total + jnp.sum(
            cotangent[0, t, 0].astype(jnp.float32) * sent[t].astype(jnp.float32),
            axis=0,
            keepdims=True,
        )
    state = updated(state, gain, sent[0])
    total, state, middle = lax.optimization_barrier((near_dp_sum(total), state, sent[1]))
    state = shifted(state, "section", 2)
    middle = shifted(middle, "section", 1)
    total = far_dp_sum(total)
    state = updated(updated(state, gain_before, middle), gain, sent[2])
    return (state[None, None], total)


def solution(mesh):
    in_specs = (
        P("dp", "section", None, None),
        P("dp", "section", None, None, None),
        P("dp", "section"),
        P("dp", "section"),
        P(),
        P("section", None),
        P("dp", None, "section", None, None),
    )
    out_specs = (P("dp", "section", None, None), P("section", None))
    return jax.shard_map(
        per_device, mesh=mesh, in_specs=in_specs, out_specs=out_specs, check_vma=False
    )
```

```python
import functools

import jax
import jax.numpy as jnp
from jax import lax
from jax.experimental import pallas as pl
from jax.experimental.pallas import tpu as pltpu
from jax.sharding import PartitionSpec as P

HD = 256
STEPS = 3
LEAST_OFFSET = 3
LANES = 128
CORES = 2
ROWS_Y = 4
VMEM = pl.BlockSpec(memory_space=pltpu.VMEM)
HBM = pl.BlockSpec(memory_space=pltpu.HBM)


def shifted(value, axis, steps):
    count = lax.axis_size(axis)
    pairs = [(source, (source + steps) % count) for source in range(count)]
    return lax.ppermute(value, axis, pairs)


def pack_kernel(length_ref, state_ref, gain_ref, message_ref, wide_ref):
    blocks = state_ref.shape[1] // LANES
    for b in range(blocks):
        message_ref[b] = state_ref[:, b * LANES : (b + 1) * LANES]
    wide = gain_ref[...].astype(jnp.float32)
    wide_ref[...] = wide
    rows = [wide[:, b * LANES : (b + 1) * LANES] for b in range(blocks)]
    message_ref[blocks] = jnp.concatenate(rows, axis=0).astype(jnp.bfloat16)
    length = length_ref[...].astype(jnp.float32)
    message_ref[blocks + 1] = jnp.broadcast_to(length, message_ref.shape[1:]).astype(jnp.bfloat16)


def packed(states, gain, length):
    rows, width = states.shape
    blocks = width // LANES
    return pl.pallas_call(
        pack_kernel,
        out_shape=[
            jax.ShapeDtypeStruct((blocks + 2, rows, LANES), states.dtype),
            jax.ShapeDtypeStruct(gain.shape, jnp.float32),
        ],
        in_specs=[VMEM] * 3,
        out_specs=[VMEM] * 2,
        name="pack",
    )(length, states, gain)


def steps_kernel(key_len_ref, message_ref, gain_next_ref, held_ref, *refs):
    out_refs, (score_ref, state_ref, memory_ref, arrival) = refs[:STEPS], refs[STEPS:]
    fetches = [
        pltpu.make_async_copy(held_ref.at[half], memory_ref.at[half], arrival.at[half])
        for half in range(2)
    ]
    fetches[0].start()
    rows = message_ref.shape[1]
    width = memory_ref.shape[2]
    heads, keys = width // HD, memory_ref.shape[1]
    blocks = width // LANES
    per_head = HD // LANES
    key_live = lax.broadcasted_iota(jnp.int32, (rows, keys), 1) < key_len_ref[...]
    length = message_ref[blocks + 1][:, :1].astype(jnp.float32)
    row_live = lax.broadcasted_iota(jnp.int32, (rows, 1), 0).astype(jnp.float32) < length
    for t in range(STEPS):
        source = message_ref if t == 0 else state_ref
        squares = jnp.zeros((rows, LANES), jnp.float32)
        for b in range(blocks):
            wide = source[b].astype(jnp.float32)
            squares = squares + wide * wide
        mean = jnp.sum(squares, axis=1, keepdims=True) / width
        scale = lax.rsqrt(mean + 1e-06)
        if t == 0:
            fetches[0].wait()
            fetches[1].start()
        for h in range(heads):
            query = jnp.concatenate(
                [
                    (source[h * per_head + j].astype(jnp.float32) * scale).astype(jnp.bfloat16)
                    for j in range(per_head)
                ],
                axis=1,
            )
            scores = lax.dot_general(
                query,
                memory_ref[0, :, h * HD : (h + 1) * HD],
                (((1,), (1,)), ((), ())),
                preferred_element_type=jnp.float32,
            )
            score_ref[h] = jnp.where(key_live, scores * HD ** (-0.5), jnp.float32(-1e30))
        if t == 0:
            fetches[1].wait()
        for h in range(heads):
            scores = score_ref[h]
            expo = jnp.exp(scores - jnp.max(scores, axis=1, keepdims=True))
            probs = (expo / jnp.sum(expo, axis=1, keepdims=True)).astype(jnp.bfloat16)
            mixed = jnp.dot(
                probs,
                memory_ref[1, :, h * HD : (h + 1) * HD],
                preferred_element_type=jnp.float32,
            ).astype(jnp.bfloat16)
            mixed = jnp.where(row_live, mixed.astype(jnp.float32), 0.0)
            attended_ref = out_refs[t].at[0] if t + 1 == STEPS else out_refs[t]
            attended_ref[:, h * HD : (h + 1) * HD] = mixed.astype(jnp.bfloat16)
            if t + 1 == STEPS:
                for j in range(per_head):
                    b = h * per_head + j
                    out_refs[t][1, :, b * LANES : (b + 1) * LANES] = source[b]
            else:
                for j in range(per_head):
                    b = h * per_head + j
                    if t == 0:
                        gain = message_ref[blocks][b : b + 1, :]
                    else:
                        gain = gain_next_ref[:, b * LANES : (b + 1) * LANES]
                    state_ref[b] = (
                        source[b].astype(jnp.float32)
                        + gain.astype(jnp.float32) * mixed[:, j * LANES : (j + 1) * LANES]
                    ).astype(jnp.bfloat16)


def attended_steps(message, gain_next, memory, key_len):
    rows = message.shape[1]
    keys, width = memory.shape[1:]
    return pl.pallas_call(
        steps_kernel,
        out_shape=[
            jax.ShapeDtypeStruct((2,) * (t + 1 == STEPS) + (rows, width), jnp.bfloat16)
            for t in range(STEPS)
        ],
        in_specs=[VMEM, VMEM, VMEM, HBM],
        out_specs=[VMEM] * STEPS,
        scratch_shapes=[
            pltpu.VMEM((width // HD, rows, keys), jnp.float32),
            pltpu.VMEM((width // LANES, rows, LANES), jnp.bfloat16),
            pltpu.VMEM(memory.shape, memory.dtype),
            pltpu.SemaphoreType.DMA((2,)),
        ],
        compiler_params=pltpu.CompilerParams(vmem_limit_bytes=16 << 20),
        name="steps",
    )(key_len, message, gain_next, memory)


def updated(state, gain_wide, attended):
    return (
        state.astype(jnp.float32) + gain_wide * attended.astype(jnp.float32)
    ).astype(jnp.bfloat16)


def by_offset(offset_index, sections, send, *operands):
    return lax.switch(
        offset_index,
        [functools.partial(send, c) for c in range(LEAST_OFFSET, sections)],
        *operands,
    )


def to_owner(offset, message, gain):
    message = shifted(message, "section", offset)
    return message, shifted(gain, "section", offset - 1)


def gain_part(cotangent, attended):
    return sum(
        jnp.sum(c.astype(jnp.float32) * a.astype(jnp.float32), axis=0, keepdims=True)
        for c, a in zip(cotangent, attended)
    )


def from_owner(offset, first, middle, last, cotangent, gain_wide):
    first = shifted(first, "section", -offset)
    middle = shifted(middle, "section", 1 - offset)
    last = shifted(last, "section", 2 - offset)
    return updated(last[1], gain_wide, last[0]), gain_part(cotangent, (first, middle, last[0]))


def near_dp_sum(row):
    count = lax.axis_size("dp")
    runs = count // (ROWS_Y * CORES)
    groups = [
        [(y * runs + run) * CORES + core for y in range(ROWS_Y) for core in range(CORES)]
        for run in range(runs)
    ]
    copies = jnp.broadcast_to(row, (ROWS_Y * CORES, row.shape[1]))
    return jnp.sum(
        lax.all_to_all(copies, "dp", 0, 0, axis_index_groups=groups), axis=0, keepdims=True
    )


def far_dp_sum(row):
    count = lax.axis_size("dp")
    runs = count // (ROWS_Y * CORES)
    groups = [
        [(y * runs + run) * CORES + core for run in range(runs)]
        for y in range(ROWS_Y)
        for core in range(CORES)
    ]
    return lax.psum(row, "dp", axis_index_groups=groups)


def per_device(states, memory, memory_len, decode_len, owner_map, section_gain, cotangent):
    sections = lax.axis_size("section")
    state, gain = states[0, 0], section_gain
    offset_index = owner_map[0] - LEAST_OFFSET

    message, gain_wide = packed(state, gain, decode_len)
    message, gain_next = by_offset(offset_index, sections, to_owner, message, gain)
    held = pltpu.with_memory_space_constraint(memory[0, 0], pltpu.HBM)
    sent = attended_steps(message, gain_next, held, memory_len)
    state, total = by_offset(
        offset_index, sections, from_owner, *sent, cotangent[0, :, 0], gain_wide
    )
    return (state[None, None], far_dp_sum(near_dp_sum(total)))


def solution(mesh):
    in_specs = (
        P("dp", "section", None, None),
        P("dp", "section", None, None, None),
        P("dp", "section"),
        P("dp", "section"),
        P(),
        P("section", None),
        P("dp", None, "section", None, None),
    )
    out_specs = (P("dp", "section", None, None), P("section", None))
    return jax.shard_map(
        per_device, mesh=mesh, in_specs=in_specs, out_specs=out_specs, check_vma=False
    )
```

```python
import functools

import jax
import jax.numpy as jnp
from jax import lax
from jax.experimental import pallas as pl
from jax.experimental.pallas import tpu as pltpu
from jax.sharding import PartitionSpec as P

HD = 256
STEPS = 3
LEAST_OFFSET = 3
LANES = 128
CORES = 2
CHUNKS = 4
ROWS_Y = 4
VMEM = pl.BlockSpec(memory_space=pltpu.VMEM)
HBM = pl.BlockSpec(memory_space=pltpu.HBM)


def shifted(value, axis, steps):
    count = lax.axis_size(axis)
    pairs = [(source, (source + steps) % count) for source in range(count)]
    return lax.ppermute(value, axis, pairs)


def pack_kernel(length_ref, state_ref, gain_ref, message_ref, wide_ref):
    blocks = state_ref.shape[1] // LANES
    for b in range(blocks):
        message_ref[b] = state_ref[:, b * LANES : (b + 1) * LANES]
    wide = gain_ref[...].astype(jnp.float32)
    wide_ref[...] = wide
    rows = [wide[:, b * LANES : (b + 1) * LANES] for b in range(blocks)]
    message_ref[blocks] = jnp.concatenate(rows, axis=0).astype(jnp.bfloat16)
    length = length_ref[...].astype(jnp.float32)
    message_ref[blocks + 1] = jnp.broadcast_to(length, message_ref.shape[1:]).astype(jnp.bfloat16)


def packed(states, gain, length):
    rows, width = states.shape
    blocks = width // LANES
    return pl.pallas_call(
        pack_kernel,
        out_shape=[
            jax.ShapeDtypeStruct((blocks + 2, rows, LANES), states.dtype),
            jax.ShapeDtypeStruct(gain.shape, jnp.float32),
        ],
        in_specs=[VMEM] * 3,
        out_specs=[VMEM] * 2,
        name="pack",
    )(length, states, gain)


def steps_kernel(key_len_ref, message_ref, gain_next_ref, held_ref, *refs):
    out_refs, (score_ref, state_ref, memory_ref, arrival) = refs[:STEPS], refs[STEPS:]
    chunk = memory_ref.shape[2] // CHUNKS
    fetches = [
        pltpu.make_async_copy(
            held_ref.at[half, :, pl.ds(part * chunk, chunk)],
            memory_ref.at[half, :, pl.ds(part * chunk, chunk)],
            arrival.at[half * CHUNKS + part],
        )
        for half in range(2)
        for part in range(CHUNKS)
    ]
    for fetch in fetches:
        fetch.start()
    rows = message_ref.shape[1]
    width = memory_ref.shape[2]
    heads, keys = width // HD, memory_ref.shape[1]
    blocks = width // LANES
    per_head = HD // LANES
    key_live = lax.broadcasted_iota(jnp.int32, (rows, keys), 1) < key_len_ref[...]
    length = message_ref[blocks + 1][:, :1].astype(jnp.float32)
    row_live = lax.broadcasted_iota(jnp.int32, (rows, 1), 0).astype(jnp.float32) < length
    for t in range(STEPS):
        source = message_ref if t == 0 else state_ref
        squares = jnp.zeros((rows, LANES), jnp.float32)
        for b in range(blocks):
            wide = source[b].astype(jnp.float32)
            squares = squares + wide * wide
        mean = jnp.sum(squares, axis=1, keepdims=True) / width
        scale = lax.rsqrt(mean + 1e-06)
        for h in range(heads):
            if t == 0 and h * HD % chunk == 0:
                fetches[h * HD // chunk].wait()
            query = jnp.concatenate(
                [
                    (source[h * per_head + j].astype(jnp.float32) * scale).astype(jnp.bfloat16)
                    for j in range(per_head)
                ],
                axis=1,
            )
            scores = lax.dot_general(
                query,
                memory_ref[0, :, h * HD : (h + 1) * HD],
                (((1,), (1,)), ((), ())),
                preferred_element_type=jnp.float32,
            )
            score_ref[h] = jnp.where(key_live, scores * HD ** (-0.5), jnp.float32(-1e30))
        for h in range(heads):
            if t == 0 and h * HD % chunk == 0:
                fetches[CHUNKS + h * HD // chunk].wait()
            scores = score_ref[h]
            expo = jnp.exp(scores - jnp.max(scores, axis=1, keepdims=True))
            probs = (expo / jnp.sum(expo, axis=1, keepdims=True)).astype(jnp.bfloat16)
            mixed = jnp.dot(
                probs,
                memory_ref[1, :, h * HD : (h + 1) * HD],
                preferred_element_type=jnp.float32,
            ).astype(jnp.bfloat16)
            mixed = jnp.where(row_live, mixed.astype(jnp.float32), 0.0)
            attended_ref = out_refs[t].at[0] if t + 1 == STEPS else out_refs[t]
            attended_ref[:, h * HD : (h + 1) * HD] = mixed.astype(jnp.bfloat16)
            if t + 1 == STEPS:
                for j in range(per_head):
                    b = h * per_head + j
                    out_refs[t][1, :, b * LANES : (b + 1) * LANES] = source[b]
            else:
                for j in range(per_head):
                    b = h * per_head + j
                    if t == 0:
                        gain = message_ref[blocks][b : b + 1, :]
                    else:
                        gain = gain_next_ref[:, b * LANES : (b + 1) * LANES]
                    state_ref[b] = (
                        source[b].astype(jnp.float32)
                        + gain.astype(jnp.float32) * mixed[:, j * LANES : (j + 1) * LANES]
                    ).astype(jnp.bfloat16)


def attended_steps(message, gain_next, memory, key_len):
    rows = message.shape[1]
    keys, width = memory.shape[1:]
    return pl.pallas_call(
        steps_kernel,
        out_shape=[
            jax.ShapeDtypeStruct((2,) * (t + 1 == STEPS) + (rows, width), jnp.bfloat16)
            for t in range(STEPS)
        ],
        in_specs=[VMEM, VMEM, VMEM, HBM],
        out_specs=[VMEM] * STEPS,
        scratch_shapes=[
            pltpu.VMEM((width // HD, rows, keys), jnp.float32),
            pltpu.VMEM((width // LANES, rows, LANES), jnp.bfloat16),
            pltpu.VMEM(memory.shape, memory.dtype),
            pltpu.SemaphoreType.DMA((2 * CHUNKS,)),
        ],
        compiler_params=pltpu.CompilerParams(vmem_limit_bytes=16 << 20),
        name="steps",
    )(key_len, message, gain_next, memory)


def updated(state, gain_wide, attended):
    return (
        state.astype(jnp.float32) + gain_wide * attended.astype(jnp.float32)
    ).astype(jnp.bfloat16)


def by_offset(offset_index, sections, send, *operands):
    return lax.switch(
        offset_index,
        [functools.partial(send, c) for c in range(LEAST_OFFSET, sections)],
        *operands,
    )


def to_owner(offset, message, gain):
    message = shifted(message, "section", offset)
    return message, shifted(gain, "section", offset - 1)


def gain_part(cotangent, attended):
    return sum(
        jnp.sum(c.astype(jnp.float32) * a.astype(jnp.float32), axis=0, keepdims=True)
        for c, a in zip(cotangent, attended)
    )


def from_owner(offset, first, middle, last, cotangent, gain_wide):
    first = shifted(first, "section", -offset)
    middle = shifted(middle, "section", 1 - offset)
    last = shifted(last, "section", 2 - offset)
    return updated(last[1], gain_wide, last[0]), gain_part(cotangent, (first, middle, last[0]))


def near_dp_sum(row):
    count = lax.axis_size("dp")
    runs = count // (ROWS_Y * CORES)
    groups = [
        [(y * runs + run) * CORES + core for y in range(ROWS_Y) for core in range(CORES)]
        for run in range(runs)
    ]
    copies = jnp.broadcast_to(row, (ROWS_Y * CORES, row.shape[1]))
    return jnp.sum(
        lax.all_to_all(copies, "dp", 0, 0, axis_index_groups=groups), axis=0, keepdims=True
    )


def far_dp_sum(row):
    count = lax.axis_size("dp")
    runs = count // (ROWS_Y * CORES)
    groups = [
        [(y * runs + run) * CORES + core for run in range(runs)]
        for y in range(ROWS_Y)
        for core in range(CORES)
    ]
    return lax.psum(row, "dp", axis_index_groups=groups)


def per_device(states, memory, memory_len, decode_len, owner_map, section_gain, cotangent):
    sections = lax.axis_size("section")
    state, gain = states[0, 0], section_gain
    offset_index = owner_map[0] - LEAST_OFFSET

    message, gain_wide = packed(state, gain, decode_len)
    message, gain_next = by_offset(offset_index, sections, to_owner, message, gain)
    held = pltpu.with_memory_space_constraint(memory[0, 0], pltpu.HBM)
    sent = attended_steps(message, gain_next, held, memory_len)
    state, total = by_offset(
        offset_index, sections, from_owner, *sent, cotangent[0, :, 0], gain_wide
    )
    return (state[None, None], far_dp_sum(near_dp_sum(total)))


def solution(mesh):
    in_specs = (
        P("dp", "section", None, None),
        P("dp", "section", None, None, None),
        P("dp", "section"),
        P("dp", "section"),
        P(),
        P("section", None),
        P("dp", None, "section", None, None),
    )
    out_specs = (P("dp", "section", None, None), P("section", None))
    return jax.shard_map(
        per_device, mesh=mesh, in_specs=in_specs, out_specs=out_specs, check_vma=False
    )
```

```python
import functools

import jax
import jax.numpy as jnp
from jax import lax
from jax.experimental import pallas as pl
from jax.experimental.pallas import tpu as pltpu
from jax.sharding import PartitionSpec as P

HD = 256
STEPS = 3
LEAST_OFFSET = 3
LANES = 128
CORES = 2
ROWS_Y = 4
VMEM = pl.BlockSpec(memory_space=pltpu.VMEM)


def shifted(value, axis, steps):
    count = lax.axis_size(axis)
    pairs = [(source, (source + steps) % count) for source in range(count)]
    return lax.ppermute(value, axis, pairs)


def pack_kernel(length_ref, state_ref, gain_ref, message_ref, wide_ref):
    blocks = state_ref.shape[1] // LANES
    for b in range(blocks):
        message_ref[b] = state_ref[:, b * LANES : (b + 1) * LANES]
    wide = gain_ref[...].astype(jnp.float32)
    wide_ref[...] = wide
    rows = [wide[:, b * LANES : (b + 1) * LANES] for b in range(blocks)]
    message_ref[blocks] = jnp.concatenate(rows, axis=0).astype(jnp.bfloat16)
    length = length_ref[...].astype(jnp.float32)
    message_ref[blocks + 1] = jnp.broadcast_to(length, message_ref.shape[1:]).astype(jnp.bfloat16)


def packed(states, gain, length):
    rows, width = states.shape
    blocks = width // LANES
    return pl.pallas_call(
        pack_kernel,
        out_shape=[
            jax.ShapeDtypeStruct((blocks + 2, rows, LANES), states.dtype),
            jax.ShapeDtypeStruct(gain.shape, jnp.float32),
        ],
        in_specs=[VMEM] * 3,
        out_specs=[VMEM] * 2,
        name="pack",
    )(length, states, gain)


def steps_kernel(key_len_ref, message_ref, gain_next_ref, memory_ref, *refs):
    out_refs, (score_ref, state_ref) = refs[:STEPS], refs[STEPS:]
    rows = message_ref.shape[1]
    width = memory_ref.shape[2]
    heads, keys = width // HD, memory_ref.shape[1]
    blocks = width // LANES
    per_head = HD // LANES
    key_live = lax.broadcasted_iota(jnp.int32, (rows, keys), 1) < key_len_ref[...]
    length = message_ref[blocks + 1][:, :1].astype(jnp.float32)
    row_live = lax.broadcasted_iota(jnp.int32, (rows, 1), 0).astype(jnp.float32) < length
    for t in range(STEPS):
        source = message_ref if t == 0 else state_ref
        squares = jnp.zeros((rows, LANES), jnp.float32)
        for b in range(blocks):
            wide = source[b].astype(jnp.float32)
            squares = squares + wide * wide
        mean = jnp.sum(squares, axis=1, keepdims=True) / width
        scale = lax.rsqrt(mean + 1e-06)
        for h in range(heads):
            query = jnp.concatenate(
                [
                    (source[h * per_head + j].astype(jnp.float32) * scale).astype(jnp.bfloat16)
                    for j in range(per_head)
                ],
                axis=1,
            )
            scores = lax.dot_general(
                query,
                memory_ref[0, :, h * HD : (h + 1) * HD],
                (((1,), (1,)), ((), ())),
                preferred_element_type=jnp.float32,
            )
            score_ref[h] = jnp.where(key_live, scores * HD ** (-0.5), jnp.float32(-1e30))
        for h in range(heads):
            scores = score_ref[h]
            expo = jnp.exp(scores - jnp.max(scores, axis=1, keepdims=True))
            probs = (expo / jnp.sum(expo, axis=1, keepdims=True)).astype(jnp.bfloat16)
            mixed = jnp.dot(
                probs,
                memory_ref[1, :, h * HD : (h + 1) * HD],
                preferred_element_type=jnp.float32,
            ).astype(jnp.bfloat16)
            mixed = jnp.where(row_live, mixed.astype(jnp.float32), 0.0)
            attended_ref = out_refs[t].at[0] if t + 1 == STEPS else out_refs[t]
            attended_ref[:, h * HD : (h + 1) * HD] = mixed.astype(jnp.bfloat16)
            if t + 1 == STEPS:
                for j in range(per_head):
                    b = h * per_head + j
                    out_refs[t][1, :, b * LANES : (b + 1) * LANES] = source[b]
            else:
                for j in range(per_head):
                    b = h * per_head + j
                    if t == 0:
                        gain = message_ref[blocks][b : b + 1, :]
                    else:
                        gain = gain_next_ref[:, b * LANES : (b + 1) * LANES]
                    state_ref[b] = (
                        source[b].astype(jnp.float32)
                        + gain.astype(jnp.float32) * mixed[:, j * LANES : (j + 1) * LANES]
                    ).astype(jnp.bfloat16)


def attended_steps(message, gain_next, memory, key_len):
    rows = message.shape[1]
    keys, width = memory.shape[1:]
    return pl.pallas_call(
        steps_kernel,
        out_shape=[
            jax.ShapeDtypeStruct((2,) * (t + 1 == STEPS) + (rows, width), jnp.bfloat16)
            for t in range(STEPS)
        ],
        in_specs=[VMEM] * 4,
        out_specs=[VMEM] * STEPS,
        scratch_shapes=[
            pltpu.VMEM((width // HD, rows, keys), jnp.float32),
            pltpu.VMEM((width // LANES, rows, LANES), jnp.bfloat16),
        ],
        compiler_params=pltpu.CompilerParams(vmem_limit_bytes=16 << 20),
        name="steps",
    )(key_len, message, gain_next, memory)


def updated(state, gain_wide, attended):
    return (
        state.astype(jnp.float32) + gain_wide * attended.astype(jnp.float32)
    ).astype(jnp.bfloat16)


def by_offset(offset_index, sections, send, *operands):
    return lax.switch(
        offset_index,
        [functools.partial(send, c) for c in range(LEAST_OFFSET, sections)],
        *operands,
    )


def to_owner(offset, message, gain, memory, key_len):
    message = shifted(message, "section", offset)
    gain_next = shifted(gain, "section", offset - 1)
    rows = lax.broadcasted_iota(jnp.int32, memory.shape, 1)
    return message, gain_next, jnp.where(rows < key_len[0, 0], memory, jnp.bfloat16(0))


def gain_part(cotangent, attended):
    return sum(
        jnp.sum(c.astype(jnp.float32) * a.astype(jnp.float32), axis=0, keepdims=True)
        for c, a in zip(cotangent, attended)
    )


def from_owner(offset, first, middle, last, cotangent, gain_wide):
    first = shifted(first, "section", -offset)
    middle = shifted(middle, "section", 1 - offset)
    last = shifted(last, "section", 2 - offset)
    return updated(last[1], gain_wide, last[0]), gain_part(cotangent, (first, middle, last[0]))


def near_dp_sum(row):
    count = lax.axis_size("dp")
    runs = count // (ROWS_Y * CORES)
    groups = [
        [(y * runs + run) * CORES + core for y in range(ROWS_Y) for core in range(CORES)]
        for run in range(runs)
    ]
    copies = jnp.broadcast_to(row, (ROWS_Y * CORES, row.shape[1]))
    return jnp.sum(
        lax.all_to_all(copies, "dp", 0, 0, axis_index_groups=groups), axis=0, keepdims=True
    )


def far_dp_sum(row):
    count = lax.axis_size("dp")
    runs = count // (ROWS_Y * CORES)
    groups = [
        [(y * runs + run) * CORES + core for run in range(runs)]
        for y in range(ROWS_Y)
        for core in range(CORES)
    ]
    return lax.psum(row, "dp", axis_index_groups=groups)


def per_device(states, memory, memory_len, decode_len, owner_map, section_gain, cotangent):
    sections = lax.axis_size("section")
    state, gain = states[0, 0], section_gain
    offset_index = owner_map[0] - LEAST_OFFSET

    message, gain_wide = packed(state, gain, decode_len)
    message, gain_next, held = by_offset(
        offset_index, sections, to_owner, message, gain, memory[0, 0], memory_len
    )
    sent = attended_steps(message, gain_next, held, memory_len)
    state, total = by_offset(
        offset_index, sections, from_owner, *sent, cotangent[0, :, 0], gain_wide
    )
    return (state[None, None], far_dp_sum(near_dp_sum(total)))


def solution(mesh):
    in_specs = (
        P("dp", "section", None, None),
        P("dp", "section", None, None, None),
        P("dp", "section"),
        P("dp", "section"),
        P(),
        P("section", None),
        P("dp", None, "section", None, None),
    )
    out_specs = (P("dp", "section", None, None), P("section", None))
    return jax.shard_map(
        per_device, mesh=mesh, in_specs=in_specs, out_specs=out_specs, check_vma=False
    )
```

```python
import functools

import jax
import jax.numpy as jnp
from jax import lax
from jax.experimental import pallas as pl
from jax.experimental.pallas import tpu as pltpu
from jax.sharding import PartitionSpec as P

HD = 256
STEPS = 3
LEAST_OFFSET = 3
LANES = 128
CORES = 2
ROWS_Y = 4
VMEM = pl.BlockSpec(memory_space=pltpu.VMEM)


def shifted(value, axis, steps):
    count = lax.axis_size(axis)
    pairs = [(source, (source + steps) % count) for source in range(count)]
    return lax.ppermute(value, axis, pairs)


def pack_kernel(length_ref, state_ref, gain_ref, message_ref, wide_ref):
    blocks = state_ref.shape[1] // LANES
    for b in range(blocks):
        message_ref[b] = state_ref[:, b * LANES : (b + 1) * LANES]
    wide = gain_ref[...].astype(jnp.float32)
    wide_ref[...] = wide
    rows = [wide[:, b * LANES : (b + 1) * LANES] for b in range(blocks)]
    message_ref[blocks] = jnp.concatenate(rows, axis=0).astype(jnp.bfloat16)
    length = length_ref[...].astype(jnp.float32)
    message_ref[blocks + 1] = jnp.broadcast_to(length, message_ref.shape[1:]).astype(jnp.bfloat16)


def packed(states, gain, length):
    rows, width = states.shape
    blocks = width // LANES
    return pl.pallas_call(
        pack_kernel,
        out_shape=[
            jax.ShapeDtypeStruct((blocks + 2, rows, LANES), states.dtype),
            jax.ShapeDtypeStruct(gain.shape, jnp.float32),
        ],
        in_specs=[VMEM] * 3,
        out_specs=[VMEM] * 2,
        name="pack",
    )(length, states, gain)


def steps_kernel(key_len_ref, message_ref, gain_next_ref, memory_ref, *refs):
    out_refs, (score_ref, state_ref) = refs[:STEPS], refs[STEPS:]
    rows = message_ref.shape[1]
    width = memory_ref.shape[2]
    heads, keys = width // HD, memory_ref.shape[1]
    blocks = width // LANES
    per_head = HD // LANES
    key_live = lax.broadcasted_iota(jnp.int32, (rows, keys), 1) < key_len_ref[...]
    length = message_ref[blocks + 1][:, :1].astype(jnp.float32)
    row_live = lax.broadcasted_iota(jnp.int32, (rows, 1), 0).astype(jnp.float32) < length
    for t in range(STEPS):
        source = message_ref if t == 0 else state_ref
        squares = jnp.zeros((rows, LANES), jnp.float32)
        for b in range(blocks):
            wide = source[b].astype(jnp.float32)
            squares = squares + wide * wide
        mean = jnp.sum(squares, axis=1, keepdims=True) / width
        scale = lax.rsqrt(mean + 1e-06)
        for h in range(heads):
            query = jnp.concatenate(
                [
                    (source[h * per_head + j].astype(jnp.float32) * scale).astype(jnp.bfloat16)
                    for j in range(per_head)
                ],
                axis=1,
            )
            scores = lax.dot_general(
                query,
                memory_ref[0, :, h * HD : (h + 1) * HD],
                (((1,), (1,)), ((), ())),
                preferred_element_type=jnp.float32,
            )
            score_ref[h] = jnp.where(key_live, scores * HD ** (-0.5), jnp.float32(-1e30))
        for h in range(heads):
            scores = score_ref[h]
            expo = jnp.exp(scores - jnp.max(scores, axis=1, keepdims=True))
            probs = (expo / jnp.sum(expo, axis=1, keepdims=True)).astype(jnp.bfloat16)
            mixed = jnp.dot(
                probs,
                memory_ref[1, :, h * HD : (h + 1) * HD],
                preferred_element_type=jnp.float32,
            ).astype(jnp.bfloat16)
            mixed = jnp.where(row_live, mixed.astype(jnp.float32), 0.0)
            attended_ref = out_refs[t].at[0] if t + 1 == STEPS else out_refs[t]
            attended_ref[:, h * HD : (h + 1) * HD] = mixed.astype(jnp.bfloat16)
            if t + 1 == STEPS:
                for j in range(per_head):
                    b = h * per_head + j
                    out_refs[t][1, :, b * LANES : (b + 1) * LANES] = source[b]
            else:
                for j in range(per_head):
                    b = h * per_head + j
                    if t == 0:
                        gain = message_ref[blocks][b : b + 1, :]
                    else:
                        gain = gain_next_ref[:, b * LANES : (b + 1) * LANES]
                    state_ref[b] = (
                        source[b].astype(jnp.float32)
                        + gain.astype(jnp.float32) * mixed[:, j * LANES : (j + 1) * LANES]
                    ).astype(jnp.bfloat16)


def attended_steps(message, gain_next, memory, key_len):
    rows = message.shape[1]
    keys, width = memory.shape[1:]
    return pl.pallas_call(
        steps_kernel,
        out_shape=[
            jax.ShapeDtypeStruct((2,) * (t + 1 == STEPS) + (rows, width), jnp.bfloat16)
            for t in range(STEPS)
        ],
        in_specs=[VMEM] * 4,
        out_specs=[VMEM] * STEPS,
        scratch_shapes=[
            pltpu.VMEM((width // HD, rows, keys), jnp.float32),
            pltpu.VMEM((width // LANES, rows, LANES), jnp.bfloat16),
        ],
        compiler_params=pltpu.CompilerParams(vmem_limit_bytes=16 << 20),
        name="steps",
    )(key_len, message, gain_next, memory)


def updated(state, gain_wide, attended):
    return (
        state.astype(jnp.float32) + gain_wide * attended.astype(jnp.float32)
    ).astype(jnp.bfloat16)


def by_offset(offset_index, sections, send, *operands):
    return lax.switch(
        offset_index,
        [functools.partial(send, c) for c in range(LEAST_OFFSET, sections)],
        *operands,
    )


def to_owner(offset, message, gain, memory, key_len):
    message = shifted(message, "section", offset)
    gain_next = shifted(gain, "section", offset - 1)
    rows = lax.broadcasted_iota(jnp.int32, memory.shape, 1)
    return message, gain_next, jnp.where(rows < key_len[0, 0], memory, jnp.bfloat16(0))


def gain_part(cotangent, attended):
    return sum(
        jnp.sum(c.astype(jnp.float32) * a.astype(jnp.float32), axis=0, keepdims=True)
        for c, a in zip(cotangent, attended)
    )


def from_owner(offset, first, middle, last, cotangent, gain_wide):
    first = shifted(first, "section", -offset)
    middle = shifted(middle, "section", 1 - offset)
    last = shifted(last, "section", 2 - offset)
    return updated(last[1], gain_wide, last[0]), gain_part(cotangent, (first, middle, last[0]))


def near_dp_sum(row):
    count = lax.axis_size("dp")
    runs = count // (ROWS_Y * CORES)
    groups = [
        [(y * runs + run) * CORES + core for y in range(ROWS_Y) for core in range(CORES)]
        for run in range(runs)
    ]
    copies = jnp.broadcast_to(row, (ROWS_Y * CORES, row.shape[1]))
    return jnp.sum(
        lax.all_to_all(copies, "dp", 0, 0, axis_index_groups=groups), axis=0, keepdims=True
    )


def far_dp_sum(row):
    count = lax.axis_size("dp")
    runs = count // (ROWS_Y * CORES)

    def target(source, step):
        y, rest = divmod(source, runs * CORES)
        run, core = divmod(rest, CORES)
        return (y * runs + (run + step) % runs) * CORES + core

    arrived = [
        lax.ppermute(row, "dp", [(s, target(s, step)) for s in range(count)])
        for step in sorted(range(1, runs), key=lambda step: -min(step, runs - step))
    ]
    return sum(arrived, row)


def per_device(states, memory, memory_len, decode_len, owner_map, section_gain, cotangent):
    sections = lax.axis_size("section")
    state, gain = states[0, 0], section_gain
    offset_index = owner_map[0] - LEAST_OFFSET

    message, gain_wide = packed(state, gain, decode_len)
    message, gain_next, held = by_offset(
        offset_index, sections, to_owner, message, gain, memory[0, 0], memory_len
    )
    sent = attended_steps(message, gain_next, held, memory_len)
    state, total = by_offset(
        offset_index, sections, from_owner, *sent, cotangent[0, :, 0], gain_wide
    )
    return (state[None, None], far_dp_sum(near_dp_sum(total)))


def solution(mesh):
    in_specs = (
        P("dp", "section", None, None),
        P("dp", "section", None, None, None),
        P("dp", "section"),
        P("dp", "section"),
        P(),
        P("section", None),
        P("dp", None, "section", None, None),
    )
    out_specs = (P("dp", "section", None, None), P("section", None))
    return jax.shard_map(
        per_device, mesh=mesh, in_specs=in_specs, out_specs=out_specs, check_vma=False
    )
```
